32 devices in a mesh: slab: 8 (over z, y), chan: 4 (over x, core).
Axes of the slice: x: 2, y: 2, z: 4, core: 2. Of those that a mesh axis runs over, the one named last changes fastest.
Arguments:
- saved_input: float32 [512, 48, 256], P('chan', 'slab'), may hold values from -6 to 6
- pre_first: float32 [512, 48, 256], P('chan', 'slab'), may hold values from -8 to 8
- pre_second: float32 [512, 48, 256], P('chan', 'slab'), may hold values from -8 to 8
- out_grad: float32 [512, 48, 256], P('chan', 'slab'), may hold values from -12 to 12
- weight_first: float32 [27, 512, 512], P(None, 'chan'), may hold values from -0.0546875 to 0.0546875
- weight_second: float32 [27, 512, 512], P(None, 'chan'), may hold values from -0.0546875 to 0.0546875
Outputs:
- input_grad: float32 [512, 48, 256], P('chan', 'slab')
- grad_weight_first: float32 [27, 512, 512], P(None, 'chan', 'slab')
- grad_weight_second: float32 [27, 512, 512], P(None, 'chan', 'slab')
The draws below stay inside these ranges and needn't reach their ends.
All inputs are finite; a program needn't handle non-finite values.
Results may differ from the reference program's by a relative error of at most 0.00013.
Values sent between devices are 32-bit elements; how exact they have to be, the bound alone decides.
A program may use at most 320 MiB of HBM per device.

```python
import math
import jax
import jax.numpy as jnp
from jax import lax

C = 512
TAPS = 27
AREA = 256
PLANES = 48


def with_spikes(result, stream_key, source, target, blocks, factor):
    def block_of(axis_at):
        return (jnp.arange(result.shape[axis_at]) // (result.shape[axis_at] // blocks)).reshape((-1,) + (1,) * (result.ndim - 1 - axis_at))

    first = jax.random.permutation(stream_key, blocks)[block_of(target)]
    other_side = (block_of(target) + blocks // 2) % blocks
    return jnp.where((block_of(source) == first) | (block_of(source) == other_side), factor * result, result)


def block_scale(own_key, dims, shards, least, high):
    level = 1.0
    for position, blocks in shards:
        steps = jax.random.uniform(jax.random.fold_in(jax.random.fold_in(own_key, 6), position), (blocks,), jnp.float32, least / len(shards), high / len(shards))
        level = level * jnp.repeat(jnp.exp(steps), dims[position] // blocks).reshape((-1,) + (1,) * (len(dims) - 1 - position))
    return level


def scatter_about(rng, shape, scale, limit, split=(), kind=jnp.bfloat16):
    gain = block_scale(rng, shape, split, -0.22, 0.18) if split else 1.0
    array = jax.random.normal(rng, shape, jnp.float32) * scale * gain
    return jnp.minimum(jnp.maximum(array, -limit), limit).astype(kind)


def gaussian_with(stream_key, shape, width, reach, shards, heavy, dtype=jnp.bfloat16):
    drawn = width * jax.random.normal(stream_key, shape, jnp.float32)
    if shards:
        drawn = drawn * block_scale(stream_key, shape, shards, -0.22, 0.18)
    return jnp.clip(with_spikes(drawn, jax.random.fold_in(stream_key, 3), *heavy), -reach, reach).astype(dtype)


def setup_inputs(seed: int = 0) -> dict:
    splits = jax.random.split(jax.random.key(seed), 7)
    saved_input = scatter_about(splits[0], (C, PLANES, AREA), 1.0, 6.0, ((0, 4), (1, 8)), jnp.float32)
    pre_first = scatter_about(splits[1], (C, PLANES, AREA), 1.5, 8.0, ((0, 4), (1, 8)), jnp.float32)
    pre_second = scatter_about(splits[2], (C, PLANES, AREA), 1.5, 8.0, ((0, 4), (1, 8)), jnp.float32)
    out_grad = gaussian_with(splits[3], (C, PLANES, AREA), 2.0, 12.0, ((0, 4), (1, 8)), (1, 0, 8, 2.0), jnp.float32)
    weight_first = scatter_about(splits[4], (TAPS, C, C), (27 * C) ** -0.5, 0.0546875, ((1, 4),), jnp.float32)
    weight_second = scatter_about(splits[5], (TAPS, C, C), (27 * C) ** -0.5, 0.0546875, ((1, 4),), jnp.float32)
    return {"saved_input": saved_input, "pre_first": pre_first, "pre_second": pre_second, "out_grad": out_grad, "weight_first": weight_first, "weight_second": weight_second}


OFFSETS = [(depth_step, row_step, col_step) for depth_step in (-1, 0, 1) for row_step in (-1, 0, 1) for col_step in (-1, 0, 1)]

def silu_slope(values):
    sigma = jax.nn.sigmoid(values)
    return sigma * (1.0 + values * (1.0 - sigma))

def layer_back(layer_input, grad_out, weight):
    channels, planes, area_cells = layer_input.shape
    side_len = math.isqrt(area_cells)
    widths = ((0, 0), (1, 1), (1, 1), (1, 1))
    input_pad = jnp.pad(layer_input.reshape(channels, planes, side_len, side_len), widths)
    grad_pad = jnp.pad(grad_out.reshape(channels, planes, side_len, side_len), widths)
    grad_flat = grad_out.reshape(channels, planes * area_cells)
    grad_in = jnp.zeros((channels, planes * area_cells), jnp.float32)
    weight_rows = []
    for tap_index, (depth_step, row_step, col_step) in enumerate(OFFSETS):
        grad_shift = grad_pad[:, 1 - depth_step:1 - depth_step + planes, 1 - row_step:1 - row_step + side_len, 1 - col_step:1 - col_step + side_len]
        grad_in = grad_in + jnp.dot(weight[tap_index], grad_shift.reshape(channels, -1), precision=lax.Precision.HIGHEST, preferred_element_type=jnp.float32)
        input_shift = input_pad[:, 1 + depth_step:1 + depth_step + planes, 1 + row_step:1 + row_step + side_len, 1 + col_step:1 + col_step + side_len]
        weight_rows.append(lax.dot_general(input_shift.reshape(channels, -1), grad_flat, (((1,), (1,)), ((), ())), precision=lax.Precision.HIGHEST, preferred_element_type=jnp.float32))
    grad_weight = jnp.stack(weight_rows, 0) / math.sqrt(planes * area_cells)
    return (grad_in.reshape(channels, planes, area_cells), grad_weight)

def reference(saved_input, pre_first, pre_second, out_grad, weight_first, weight_second):
    hidden = jax.nn.silu(pre_first)
    second_grad = out_grad * silu_slope(pre_second)
    hidden_grad, grad_weight_second = layer_back(hidden, second_grad, weight_second)
    first_grad = hidden_grad * silu_slope(pre_first)
    input_grad, grad_weight_first = layer_back(saved_input, first_grad, weight_first)
    return (input_grad, grad_weight_first, grad_weight_second)
```

```python
import math

import jax
import jax.numpy as jnp
from jax import lax
from jax.sharding import PartitionSpec as P

STEPS = (-1, 0, 1)
IN_PLANE = [(row_step, col_step) for row_step in STEPS for col_step in STEPS]


def with_rim(value):
    count = lax.axis_size("slab")
    up = [(i, i + 1) for i in range(count - 1)]
    down = [(j, i) for i, j in up]
    before = lax.ppermute(value[-1:], "slab", up)
    after = lax.ppermute(value[:1], "slab", down)
    return jnp.concatenate([before, value, after], axis=0)


def silu_slope(values):
    sigma = jax.nn.sigmoid(values)
    return sigma * (1.0 + values * (1.0 - sigma))


def shift_cells(block, row_step, col_step, side_len):
    area_cells = block.shape[-1]
    if row_step == 0 and col_step == 0:
        return block
    cell_ids = lax.iota(jnp.int32, area_cells)
    row_ids = cell_ids // side_len
    col_ids = cell_ids % side_len
    valid = (
        (row_ids + row_step >= 0)
        & (row_ids + row_step < side_len)
        & (col_ids + col_step >= 0)
        & (col_ids + col_step < side_len)
    )
    rolled = jnp.roll(block, -(row_step * side_len + col_step), axis=-1)
    return jnp.where(valid, rolled, jnp.zeros_like(rolled))


def gather_channels(rimmed):
    planes, channels, cells = rimmed.shape
    portion = lax.all_gather(rimmed, "chan", axis=0)
    return portion.transpose(1, 0, 2, 3).reshape(planes, -1, cells)


def input_side(portion, weight, side_len):
    planes = portion.shape[0] - 2
    channels, total = weight.shape[1:]
    near = jnp.stack([portion[1 - a : 1 - a + planes] for a in STEPS], 0)
    rows = weight.reshape(len(STEPS), len(IN_PLANE) * channels, total)
    summed = lax.dot_general(
        rows,
        near,
        (((0, 2), (0, 2)), ((), ())),
        precision=lax.Precision.HIGH,
        preferred_element_type=jnp.float32,
    )
    summed = summed.reshape(len(IN_PLANE), channels, planes, -1)
    result = jnp.zeros(summed.shape[1:], jnp.float32)
    for index, (row_step, col_step) in enumerate(IN_PLANE):
        result = result + shift_cells(summed[index], -row_step, -col_step, side_len)
    return result.transpose(1, 0, 2)


def weight_side(rimmed, centre, side_len):
    planes, total, cells = centre.shape
    channels = rimmed.shape[1]
    moved = jnp.stack([shift_cells(rimmed, b, c, side_len) for b, c in IN_PLANE], 1)
    moved = moved.reshape(planes + 2, len(IN_PLANE) * channels, cells)
    voxels = planes * lax.axis_size("slab") * cells
    parts = []
    for a in STEPS:
        part = lax.dot_general(
            moved[1 + a : 1 + a + planes],
            centre,
            (((0, 2), (0, 2)), ((), ())),
            precision=lax.Precision.HIGH,
            preferred_element_type=jnp.float32,
        )
        parts.append(part.reshape(len(IN_PLANE), channels, total) / math.sqrt(voxels))
    return parts


def reduce_parts(parts):
    done = [lax.psum_scatter(part, "slab", scatter_dimension=2, tiled=True) for part in parts]
    return jnp.concatenate(done, 0)


def per_device(saved_input, pre_first, pre_second, out_grad, weight_first, weight_second):
    side_len = math.isqrt(saved_input.shape[-1])
    saved_input, pre_first, pre_second, out_grad = (
        value.transpose(1, 0, 2) for value in (saved_input, pre_first, pre_second, out_grad)
    )
    second_grad = out_grad * silu_slope(pre_second)
    second_all = gather_channels(with_rim(second_grad))
    hidden = with_rim(jax.nn.silu(pre_first))
    input_rim = with_rim(saved_input)
    hidden_grad = input_side(second_all, weight_second, side_len)
    first_grad = hidden_grad * silu_slope(pre_first)
    first_all = gather_channels(with_rim(first_grad))
    second_parts = weight_side(hidden, second_all[1:-1], side_len)
    first_all, second_parts = lax.optimization_barrier((first_all, second_parts))
    first_parts = weight_side(input_rim, first_all[1:-1], side_len)
    input_grad = input_side(first_all, weight_first, side_len)
    return (input_grad.transpose(1, 0, 2), reduce_parts(first_parts), reduce_parts(second_parts))


def solution(mesh):
    in_specs = (
        P("chan", "slab", None),
        P("chan", "slab", None),
        P("chan", "slab", None),
        P("chan", "slab", None),
        P(None, "chan", None),
        P(None, "chan", None),
    )
    out_specs = (P("chan", "slab", None), P(None, "chan", "slab"), P(None, "chan", "slab"))
    return jax.shard_map(
        per_device, mesh=mesh, in_specs=in_specs, out_specs=out_specs, check_vma=False
    )
```
